32 devices in a mesh: section: 4 (over x, core), tensor: 2 (over y), dp: 4 (over z).
Axes of the slice: x: 2, y: 2, z: 4, core: 2. Of those that a mesh axis runs over, the one named last changes fastest.
Arguments:
- residuals: bfloat16 [4, 4, 2, 128, 8192], P('section', 'dp', None, 'tensor'), may hold values from -6 to 6
- norm_gain: bfloat16 [4, 8192], P('section'), may hold values from 0.5 to 1.5
- projection: bfloat16 [4, 8192, 2, 2, 128], P('section', None, 'tensor'), may hold values from -0.0625 to 0.0625
- queries: bfloat16 [4, 4, 2, 128, 2, 1024], P('section', 'dp', None, None, 'tensor'), may hold values from -48 to 48
- output_grad: bfloat16 [4, 4, 2, 128, 2, 1024], P('section', 'dp', None, None, 'tensor'), may hold values from -6 to 6
- section_cotangent: bfloat16 [4, 4, 128, 8192], P('section', 'dp', 'tensor'), may hold values from -6 to 6
- loss_cotangent: bfloat16 [4, 128, 8192], P('dp', 'tensor'), may hold values from -6 to 6
- lengths: int32 [4, 4, 2], P('section', 'dp'), may hold values from 64 to 128
- segments: int32 [4, 4, 2, 128], P('section', 'dp'), may hold values from 0 to 2, never falling along the last dimension, each value on 1 to 64 neighbouring positions
Outputs:
- query_grad: bfloat16 [4, 4, 2, 128, 2, 1024], P('section', 'dp', None, None, 'tensor')
- residual_grad: bfloat16 [4, 4, 128, 8192], P('section', 'dp', 'tensor')
- projection_grad: bfloat16 [4, 8192, 2, 2, 128], P('section', 'dp', 'tensor')
The draws below stay inside these ranges and needn't reach their ends.
All inputs are finite; a program needn't handle non-finite values.
Results may differ from the reference program's by a relative error of at most 0.015.
Values may be sent and summed in bfloat16 or wider, within the bound.
A program may use at most 64 MiB of HBM per device.

```python
import math
import jax
import jax.numpy as jnp
import numpy as np
from jax import lax

D = 8192
HD = 128
GROUP = 8
KVH = 2
SEQ = 128
TICKS = 2
SECTIONS = 4
REPLICAS = 4


def draw_queries(key, part):
    shape = (SECTIONS, REPLICAS, TICKS, SEQ, KVH, GROUP * HD)
    base = jnp.clip(jax.random.normal(jax.random.fold_in(key, 11), shape, jnp.float32), -6.0, 6.0)
    return base.astype(jnp.bfloat16)


def set_ends(drawn, stream_key, least, high):
    longest = drawn.shape.index(max(drawn.shape))
    spots = []
    for shift in (0, 1):
        where = [jax.random.randint(jax.random.fold_in(stream_key, axis), (), 0, length) for axis, length in enumerate(drawn.shape)]
        where[longest] = (where[longest] + shift) % drawn.shape[longest]
        spots.append(tuple(where))
    return drawn.at[spots[0]].set(least).at[spots[1]].set(high)


def steps_of(stream_key, dims, cuts, least, top_value):
    factor_of, own = 1.0, jax.random.fold_in(stream_key, 6)
    for axis_at, parts in cuts:
        heights = jnp.exp(jax.random.uniform(jax.random.fold_in(own, axis_at), (parts,), jnp.float32, least / len(cuts), top_value / len(cuts)))
        factor_of = factor_of * jnp.repeat(heights, dims[axis_at] // parts).reshape([-1 if axis == axis_at else 1 for axis in range(len(dims))])
    return factor_of


def length_profile(count, total, reach, skew):
    weights = [(1 << 20) // math.isqrt(grade ** skew) + 1 for grade in range(2, count + 1)]
    surplus, holding = total - reach - (count - 1), [1] * (count - 1)
    while surplus > 0:
        movable = [i for i in range(count - 1) if holding[i] < reach]
        whole, budget = sum([weights[i] for i in movable]), surplus
        for i in movable:
            addition = min(reach - holding[i], max(1, budget * weights[i] // whole), surplus)
            holding[i] = holding[i] + addition
            surplus = surplus - addition
    return np.array([reach] + holding)


def ragged_sizes(rng, amount, total, limit, slope):
    if amount == 2:
        one = jax.random.randint(rng, (), max(1, total - limit), min(limit, total - 1) + 1)
        return jnp.stack([one, total - one])
    tallies = jnp.asarray(length_profile(amount, total, limit, slope), jnp.int32)
    pairs = (amount - 1) // 2
    giver, taker = tallies[1:1 + 2 * pairs:2], tallies[2:2 + 2 * pairs:2]
    slack = jnp.minimum(giver - 1, limit - taker)
    shifted = jax.random.randint(jax.random.fold_in(rng, 1), (pairs,), 0, 1 << 20) % (slack + 1)
    tallies = tallies.at[1:1 + 2 * pairs:2].set(giver - shifted).at[2:2 + 2 * pairs:2].set(taker + shifted)
    return tallies[jax.random.permutation(jax.random.fold_in(rng, 2), amount)]


def scatter_about(rng, extent, deviation, most, split=(), kind=jnp.bfloat16):
    values = deviation * jax.random.normal(rng, extent, jnp.float32)
    if split:
        values = values * steps_of(rng, extent, split, -0.22, 0.18)
    return jnp.clip(values, -most, most).astype(kind)


def setup_inputs(seed: int = 0) -> dict:
    seeds = jax.random.split(jax.random.key(seed), 10)
    return {
        "residuals": scatter_about(seeds[0], (SECTIONS, REPLICAS, TICKS, SEQ, D), 1.0, 6.0, ((0, 4), (1, 4), (3, 2))),
        "norm_gain": jnp.clip(1.0 + 0.1 * jax.random.normal(seeds[1], (SECTIONS, D), jnp.float32), 0.5, 1.5).astype(jnp.bfloat16),
        "projection": scatter_about(seeds[2], (SECTIONS, D, KVH, 2, HD), D ** -0.5, 0.0625, ((0, 4), (2, 2))),
        "queries": draw_queries(jax.random.fold_in(seeds[9], 71), 0),
        "output_grad": scatter_about(seeds[4], (SECTIONS, REPLICAS, TICKS, SEQ, KVH, GROUP * HD), 1.0, 6.0, ((0, 4), (1, 4), (4, 2))),
        "section_cotangent": scatter_about(seeds[5], (SECTIONS, REPLICAS, SEQ, D), 1.0, 6.0, ((0, 4), (1, 4), (2, 2))),
        "loss_cotangent": scatter_about(seeds[6], (REPLICAS, SEQ, D), 1.0, 6.0, ((0, 4), (1, 2))),
        "lengths": set_ends(jax.random.randint(seeds[7], (SECTIONS, REPLICAS, TICKS), SEQ // 2, SEQ + 1), jax.random.fold_in(seeds[7], 1), SEQ // 2, SEQ).astype(jnp.int32),
        "segments": jax.vmap(lambda own: jnp.searchsorted(jnp.cumsum(ragged_sizes(own, 3, SEQ, SEQ // 2, 1)), jnp.arange(SEQ), side="right"))(jax.random.split(seeds[8], SECTIONS * REPLICAS * TICKS)).reshape((SECTIONS, REPLICAS, TICKS, SEQ)).astype(jnp.int32),
    }


EPSILON = 1e-05
MASKED = -1e+30

def settle(tensor):
    return lax.optimization_barrier(tensor).astype(jnp.float32)

def attend_grad(query, key_rows, value_rows, masked_grad, visible):
    scaling = HD ** (-0.5)
    query_wide = settle(query)
    key_wide = settle(key_rows)
    value_wide = settle(value_rows)
    grad_wide = settle(masked_grad)
    scores = jnp.einsum('gqd,kd->gqk', query_wide, key_wide) * scaling
    scores = jnp.where(visible[None], scores, MASKED)
    row_max = lax.optimization_barrier(jnp.max(scores, axis=-1, keepdims=True))
    exponent = jnp.exp(scores - row_max)
    attention = exponent / lax.optimization_barrier(jnp.sum(exponent, axis=-1, keepdims=True))
    attention_wide = settle(attention.astype(jnp.bfloat16))
    mixed = jnp.einsum('gqk,kd->gqd', attention_wide, value_wide)
    correction = lax.optimization_barrier(jnp.sum(grad_wide * mixed, axis=-1))
    value_grad = jnp.einsum('gqk,gqd->kd', attention_wide, grad_wide)
    weight_grad = jnp.einsum('gqd,kd->gqk', grad_wide, value_wide)
    score_grad = settle((attention * (weight_grad - correction[..., None])).astype(jnp.bfloat16))
    query_grad = (jnp.einsum('gqk,kd->gqd', score_grad, key_wide) * scaling).astype(jnp.bfloat16)
    key_grad = jnp.einsum('gqk,gqd->kd', score_grad, query_wide) * scaling
    return (query_grad, jnp.concatenate([key_grad, value_grad], axis=1).astype(jnp.bfloat16))

def section_tick(residual, gain_row, weights, query_rows, grad_rows, length, segment):
    upcast = residual.astype(jnp.float32)
    inverse = lax.rsqrt(lax.optimization_barrier(jnp.mean(upcast * upcast, axis=1, keepdims=True)) + EPSILON)
    gain_wide = gain_row.astype(jnp.float32)
    normed = (upcast * inverse * gain_wide).astype(jnp.bfloat16)
    projected = jnp.dot(normed, weights, preferred_element_type=jnp.float32).astype(jnp.bfloat16)
    projected = projected.reshape(SEQ, KVH, 2, HD)
    position = jnp.arange(SEQ, dtype=jnp.int32)
    visible = (position[None, :] <= position[:, None]) & (segment[:, None] == segment[None, :])
    live_mask = (position < length).astype(jnp.bfloat16)
    masked_grad = grad_rows * live_mask[:, None, None]
    query_heads = query_rows.reshape(SEQ, KVH, GROUP, HD).transpose(1, 2, 0, 3)
    grad_heads = masked_grad.reshape(SEQ, KVH, GROUP, HD).transpose(1, 2, 0, 3)
    key_heads = projected[:, :, 0, :].transpose(1, 0, 2)
    value_heads = projected[:, :, 1, :].transpose(1, 0, 2)
    query_grad, pair_grad = jax.vmap(attend_grad, in_axes=(0, 0, 0, 0, None))(query_heads, key_heads, value_heads, grad_heads, visible)
    query_grad = query_grad.transpose(2, 0, 1, 3).reshape(SEQ, KVH, GROUP * HD)
    head_weights = weights.astype(jnp.float32).reshape(D, KVH, 2 * HD)
    partial_value = jnp.einsum('hsc,dhc->hsd', settle(pair_grad), head_weights)
    normed_grad = lax.optimization_barrier(jnp.sum(settle(partial_value.astype(jnp.bfloat16)), axis=0))
    scaled = normed_grad * gain_wide
    norm_back = inverse * scaled - upcast * inverse * inverse * inverse * lax.optimization_barrier(jnp.mean(scaled * upcast, axis=1, keepdims=True))
    pair_flat = pair_grad.transpose(1, 0, 2).reshape(SEQ, KVH * 2 * HD)
    return (query_grad, pair_flat, normed, norm_back)

def reference(residuals, norm_gain, projection, queries, output_grad, section_cotangent, loss_cotangent, lengths, segments):

    def first_pass(section_index):
        weights = projection[section_index].reshape(D, KVH * 2 * HD)

        def replica_pass(replica):
            outcome = section_tick(residuals[section_index, replica, 0], norm_gain[section_index], weights, queries[section_index, replica, 0], output_grad[section_index, replica, 0], lengths[section_index, replica, 0], segments[section_index, replica, 0])
            return (section_cotangent[section_index, replica].astype(jnp.float32) + outcome[3]).astype(jnp.bfloat16)
        return lax.map(replica_pass, jnp.arange(REPLICAS, dtype=jnp.int32))
    outgoing = lax.map(first_pass, jnp.arange(SECTIONS, dtype=jnp.int32))
    incoming = jnp.concatenate([outgoing[1:], loss_cotangent[None]], axis=0)

    def second_pass(section_index):
        weights = projection[section_index].reshape(D, KVH * 2 * HD)

        def replica_step(running, replica):
            query_list = []
            replica_sum = jnp.zeros((D, KVH * 2 * HD), jnp.float32)
            norm_last = None
            for tick_index in range(2):
                query_grad, pair_flat, normed, norm_back = section_tick(residuals[section_index, replica, tick_index], norm_gain[section_index], weights, queries[section_index, replica, tick_index], output_grad[section_index, replica, tick_index], lengths[section_index, replica, tick_index], segments[section_index, replica, tick_index])
                query_list.append(query_grad)
                replica_sum = replica_sum + jnp.dot(normed.T, pair_flat, preferred_element_type=jnp.float32)
                norm_last = norm_back
            running = running + settle(replica_sum.astype(jnp.bfloat16))
            residual_grad = (incoming[section_index, replica].astype(jnp.float32) + norm_last).astype(jnp.bfloat16)
            return (running, (jnp.stack(query_list), residual_grad))
        running, (query_all, residual_all) = lax.scan(replica_step, jnp.zeros((D, KVH * 2 * HD), jnp.float32), jnp.arange(REPLICAS, dtype=jnp.int32))
        return (running.astype(jnp.bfloat16).reshape(D, KVH, 2, HD), query_all, residual_all)
    projection_grad, query_grad, residual_grad = lax.map(second_pass, jnp.arange(SECTIONS, dtype=jnp.int32))
    return (query_grad, residual_grad, projection_grad)
```

```python
import jax
import jax.numpy as jnp
from jax import lax
from jax.sharding import PartitionSpec as P

EPSILON = 1e-05
MASKED = -1e30


def shifted(value, axis, steps):
    count = lax.axis_size(axis)
    leading, last = (max(0, -steps), min(count, count - steps))
    return lax.ppermute(value, axis, [(source, source + steps) for source in range(leading, last)])


def normalize(residual, gain_wide):
    upcast = residual.astype(jnp.float32)
    inverse = lax.rsqrt(jnp.mean(upcast * upcast, axis=-1, keepdims=True) + EPSILON)
    return ((upcast * inverse * gain_wide).astype(jnp.bfloat16), inverse)


def project(rows, weights):
    return jnp.dot(rows, weights, preferred_element_type=jnp.float32).astype(jnp.bfloat16)


def head_grads(projected, query_rows, grad_rows, length, segment):
    head_size = projected.shape[1] // 2
    row_total = projected.shape[0]
    group_size = query_rows.shape[-1] // head_size
    scaling = head_size ** (-0.5)
    key_rows = projected[:, :head_size]
    value_rows = projected[:, head_size:]
    position = lax.iota(jnp.int32, row_total)
    visible = (position[None, :] <= position[:, None]) & (segment[:, None] == segment[None, :])
    live_mask = (position < length).astype(jnp.bfloat16)
    query = query_rows.reshape(row_total, group_size, head_size)
    masked_grad = grad_rows.reshape(row_total, group_size, head_size) * live_mask[:, None, None]
    scores = (
        jnp.einsum("qgd,kd->gqk", query, key_rows, preferred_element_type=jnp.float32) * scaling
    )
    scores = jnp.where(visible[None], scores, MASKED)
    row_max = jnp.max(scores, axis=-1, keepdims=True)
    exponent = jnp.exp(scores - row_max)
    attention = exponent / jnp.sum(exponent, axis=-1, keepdims=True)
    attention_low = attention.astype(jnp.bfloat16)
    mixed = jnp.einsum("gqk,kd->gqd", attention_low, value_rows, preferred_element_type=jnp.float32)
    correction = jnp.sum(mixed * jnp.transpose(masked_grad, (1, 0, 2)).astype(jnp.float32), axis=-1)
    value_grad = jnp.einsum(
        "gqk,qgd->kd", attention_low, masked_grad, preferred_element_type=jnp.float32
    )
    weight_grad = jnp.einsum(
        "qgd,kd->gqk", masked_grad, value_rows, preferred_element_type=jnp.float32
    )
    score_grad = (attention * (weight_grad - correction[..., None])).astype(jnp.bfloat16)
    query_grad = (
        jnp.einsum("gqk,kd->qgd", score_grad, key_rows, preferred_element_type=jnp.float32)
        * scaling
    ).astype(jnp.bfloat16)
    key_grad = (
        jnp.einsum("gqk,qgd->kd", score_grad, query, preferred_element_type=jnp.float32) * scaling
    )
    pair_grad = jnp.concatenate([key_grad, value_grad], axis=1).astype(jnp.bfloat16)
    return (query_grad.reshape(row_total, 1, group_size * head_size), pair_grad)


def rotated(value, axis, steps):
    count = lax.axis_size(axis)
    return lax.ppermute(value, axis, [(source, (source + steps) % count) for source in range(count)])


def on_device(
    residuals,
    norm_gain,
    projection,
    queries,
    output_grad,
    section_cotangent,
    loss_cotangent,
    lengths,
    segments,
):
    local_rows = residuals[0, 0]
    tick_count, row_count, model_width = local_rows.shape
    head_size = projection.shape[4]
    pair_width = 2 * head_size
    weights = projection.reshape(model_width, pair_width)
    gain_wide = norm_gain[0].astype(jnp.float32)
    tensor_count = lax.axis_size("tensor")
    tensor_index = lax.axis_index("tensor")
    dp_count = lax.axis_size("dp")
    dp_index = lax.axis_index("dp")
    block_width = model_width // dp_count
    row_total = row_count * tensor_count
    ticks = range(tick_count)

    def owner_start(steps):
        return lax.rem(tensor_index + (tensor_count + steps), tensor_count) * row_count

    def column_block(value, steps):
        start = lax.rem(dp_index + steps, dp_count) * block_width
        return lax.dynamic_slice_in_dim(value, start, block_width, axis=value.ndim - 1)

    normed_ticks, inverse_ticks, arrived = [], [], []
    for tick in ticks:
        normed, inverse = normalize(local_rows[tick], gain_wide)
        normed_ticks.append(normed)
        inverse_ticks.append(inverse)
        arrived.append([rotated(normed, "tensor", k) for k in range(1, tensor_count)])
    normed_local = jnp.stack(normed_ticks)

    own_columns = [column_block(normed_local, 0)] + [
        rotated(column_block(normed_local, j), "dp", j) for j in range(1, dp_count)
    ]

    projected_own = project(normed_local.reshape(-1, model_width), weights)
    projected_own = projected_own.reshape(tick_count, row_count, pair_width)

    query_list, pair_list, received, kept = [], [], [], []
    for tick in ticks:
        projected = jnp.zeros((row_total, pair_width), jnp.bfloat16)
        pieces = [projected_own[tick]] + [project(rows, weights) for rows in arrived[tick]]
        for k, piece in enumerate(pieces):
            projected = lax.dynamic_update_slice_in_dim(projected, piece, owner_start(-k), axis=0)
        query_grad, pair_grad = head_grads(
            projected,
            queries[0, 0, tick],
            output_grad[0, 0, tick],
            lengths[0, 0, tick],
            segments[0, 0, tick],
        )
        query_list.append(query_grad)

        def partial(steps):
            rows = lax.dynamic_slice_in_dim(pair_grad, owner_start(steps), row_count, axis=0)
            return lax.dot_general(
                rows, weights, (((1,), (1,)), ((), ())), preferred_element_type=jnp.float32
            ).astype(jnp.bfloat16)

        received.append([rotated(partial(k), "tensor", k) for k in range(1, tensor_count)])
        kept.append(partial(0))
        pair_list.append(
            jnp.stack(
                [
                    lax.dynamic_slice_in_dim(pair_grad, owner_start(-k), row_count, axis=0)
                    for k in range(tensor_count)
                ]
            )
        )

    other = jnp.stack(
        [jnp.stack([arrived[tick][k] for tick in ticks]) for k in range(tensor_count - 1)]
    )
    other_columns = [column_block(other, 0)] + [
        rotated(column_block(other, j), "dp", j) for j in range(1, dp_count)
    ]
    pair_local = jnp.stack(pair_list, axis=1)
    pair_all = [pair_local] + [rotated(pair_local, "dp", j) for j in range(1, dp_count)]

    def norm_back(tick):
        normed_grad = kept[tick].astype(jnp.float32)
        for part in received[tick]:
            normed_grad = normed_grad + part.astype(jnp.float32)
        upcast = local_rows[tick].astype(jnp.float32)
        inverse = inverse_ticks[tick]
        scaled = normed_grad * gain_wide
        return inverse * scaled - upcast * inverse * inverse * inverse * jnp.mean(
            scaled * upcast, axis=-1, keepdims=True
        )

    outgoing = (section_cotangent[0, 0].astype(jnp.float32) + norm_back(0)).astype(jnp.bfloat16)
    incoming = shifted(outgoing, "section", -1)
    is_last = lax.axis_index("section") == lax.axis_size("section") - 1
    incoming = jnp.where(is_last, loss_cotangent[0], incoming)
    residual_grad = (incoming.astype(jnp.float32) + norm_back(1)).astype(jnp.bfloat16)

    def contract(columns, pairs):
        left = jnp.concatenate([value.reshape(-1, block_width) for value in columns])
        right = jnp.concatenate([value.reshape(-1, pair_width) for value in pairs])
        return lax.dot_general(
            left, right, (((0,), (0,)), ((), ())), preferred_element_type=jnp.float32
        )

    weight_sum = contract(own_columns, [value[0] for value in pair_all])
    if tensor_count > 1:
        weight_sum = weight_sum + contract(other_columns, [value[1:] for value in pair_all])
    projection_grad = weight_sum.astype(jnp.bfloat16).reshape(1, -1, 1, 2, head_size)
    query_all = jnp.stack(query_list)[None, None]
    return (query_all, residual_grad[None, None], projection_grad)


def solution(mesh):
    in_specs = (
        P("section", "dp", None, "tensor", None),
        P("section", None),
        P("section", None, "tensor", None, None),
        P("section", "dp", None, None, "tensor", None),
        P("section", "dp", None, None, "tensor", None),
        P("section", "dp", "tensor", None),
        P("dp", "tensor", None),
        P("section", "dp", None),
        P("section", "dp", None, None),
    )
    out_specs = (
        P("section", "dp", None, None, "tensor", None),
        P("section", "dp", "tensor", None),
        P("section", "dp", "tensor", None, None),
    )
    return jax.shard_map(
        on_device, mesh=mesh, in_specs=in_specs, out_specs=out_specs, check_vma=False
    )
```

```python
import jax
import jax.numpy as jnp
from jax import lax
from jax.sharding import PartitionSpec as P


EPSILON = 1e-05
MASKED = -1e30


def shifted(value, axis, steps):
    count = lax.axis_size(axis)
    leading, last = (max(0, -steps), min(count, count - steps))
    return lax.ppermute(value, axis, [(source, source + steps) for source in range(leading, last)])


def normalize(residual, gain_wide):
    upcast = residual.astype(jnp.float32)
    inverse = lax.rsqrt(jnp.mean(upcast * upcast, axis=-1, keepdims=True) + EPSILON)
    return ((upcast * inverse * gain_wide).astype(jnp.bfloat16), inverse)


def project(rows, weights):
    return jnp.dot(rows, weights, preferred_element_type=jnp.float32).astype(jnp.bfloat16)


def head_grads(projected, query_rows, grad_rows, length, segment):
    head_size = projected.shape[1] // 2
    row_total = projected.shape[0]
    group_size = query_rows.shape[-1] // head_size
    scaling = head_size ** (-0.5)
    key_rows = projected[:, :head_size]
    value_rows = projected[:, head_size:]
    position = lax.iota(jnp.int32, row_total)
    visible = (position[None, :] <= position[:, None]) & (segment[:, None] == segment[None, :])
    live_mask = (position < length).astype(jnp.bfloat16)
    query = query_rows.reshape(row_total, group_size, head_size)
    masked_grad = grad_rows.reshape(row_total, group_size, head_size) * live_mask[:, None, None]
    scores = (
        jnp.einsum("qgd,kd->gqk", query, key_rows, preferred_element_type=jnp.float32) * scaling
    )
    scores = jnp.where(visible[None], scores, MASKED)
    row_max = jnp.max(scores, axis=-1, keepdims=True)
    exponent = jnp.exp(scores - row_max)
    attention = exponent / jnp.sum(exponent, axis=-1, keepdims=True)
    attention_low = attention.astype(jnp.bfloat16)
    mixed = jnp.einsum("gqk,kd->gqd", attention_low, value_rows, preferred_element_type=jnp.float32)
    correction = jnp.sum(mixed * jnp.transpose(masked_grad, (1, 0, 2)).astype(jnp.float32), axis=-1)
    value_grad = jnp.einsum(
        "gqk,qgd->kd", attention_low, masked_grad, preferred_element_type=jnp.float32
    )
    weight_grad = jnp.einsum(
        "qgd,kd->gqk", masked_grad, value_rows, preferred_element_type=jnp.float32
    )
    score_grad = (attention * (weight_grad - correction[..., None])).astype(jnp.bfloat16)
    query_grad = (
        jnp.einsum("gqk,kd->qgd", score_grad, key_rows, preferred_element_type=jnp.float32)
        * scaling
    ).astype(jnp.bfloat16)
    key_grad = (
        jnp.einsum("gqk,qgd->kd", score_grad, query, preferred_element_type=jnp.float32) * scaling
    )
    pair_grad = jnp.concatenate([key_grad, value_grad], axis=1).astype(jnp.bfloat16)
    return (query_grad.reshape(row_total, 1, group_size * head_size), pair_grad)


def rotated(value, axis, steps):
    count = lax.axis_size(axis)
    return lax.ppermute(value, axis, [(source, (source + steps) % count) for source in range(count)])


def after(value, *earlier):
    return lax.optimization_barrier((value, *earlier))[0]


def on_device(
    residuals,
    norm_gain,
    projection,
    queries,
    output_grad,
    section_cotangent,
    loss_cotangent,
    lengths,
    segments,
):
    local_rows = residuals[0, 0]
    tick_count, row_count, model_width = local_rows.shape
    head_size = projection.shape[4]
    pair_width = 2 * head_size
    weights = projection.reshape(model_width, pair_width)
    gain_wide = norm_gain[0].astype(jnp.float32)
    tensor_count = lax.axis_size("tensor")
    tensor_index = lax.axis_index("tensor")
    dp_count = lax.axis_size("dp")
    dp_index = lax.axis_index("dp")
    block_width = model_width // dp_count
    row_total = row_count * tensor_count
    ticks = range(tick_count)

    def owner_start(steps):
        return lax.rem(tensor_index + (tensor_count + steps), tensor_count) * row_count

    def column_block(value, steps):
        start = lax.rem(dp_index + steps, dp_count) * block_width
        return lax.dynamic_slice_in_dim(value, start, block_width, axis=value.ndim - 1)

    normed_ticks, inverse_ticks, arrived = [], [], []
    for tick in ticks:
        rows = after(local_rows[tick], *normed_ticks)
        normed, inverse = normalize(rows, gain_wide)
        normed_ticks.append(normed)
        inverse_ticks.append(inverse)
        arrived.append([rotated(normed, "tensor", k) for k in range(1, tensor_count)])
    normed_local = jnp.stack(normed_ticks)

    own_columns = [column_block(normed_local, 0)] + [
        rotated(column_block(normed_local, j), "dp", j) for j in range(1, dp_count)
    ]

    projected_own = project(normed_local.reshape(-1, model_width), weights)
    projected_own = projected_own.reshape(tick_count, row_count, pair_width)

    query_list, pair_list, received, kept = [], [], [], []
    other_ticks = []
    sent = ()
    for tick in ticks:
        gathered = after(arrived[tick], *sent)
        columns = [
            [column_block(rows, j) for rows in gathered] for j in range(dp_count)
        ]
        columns = lax.optimization_barrier(columns)
        if tick > 0:
            gathered = after(gathered, columns)
        pieces = [projected_own[tick]] + [project(rows, weights) for rows in gathered]
        projected = jnp.zeros((row_total, pair_width), jnp.bfloat16)
        for k, piece in enumerate(pieces):
            projected = lax.dynamic_update_slice_in_dim(
                projected, piece, owner_start(-k), axis=0
            )
        query_grad, pair_grad = head_grads(
            projected,
            queries[0, 0, tick],
            output_grad[0, 0, tick],
            lengths[0, 0, tick],
            segments[0, 0, tick],
        )

        def partial(pairs, steps):
            rows = lax.dynamic_slice_in_dim(pairs, owner_start(steps), row_count, axis=0)
            return lax.dot_general(
                rows, weights, (((1,), (1,)), ((), ())), preferred_element_type=jnp.float32
            ).astype(jnp.bfloat16)

        leaving = [partial(pair_grad, k) for k in range(1, tensor_count)]
        leaving = lax.optimization_barrier(leaving)
        received.append([rotated(value, "tensor", k + 1) for k, value in enumerate(leaving)])
        sent = tuple(leaving)
        query_grad, pair_grad = after((query_grad, pair_grad), *sent)
        if tick == 0:
            columns = after(columns, *sent)
        other_ticks.append(
            [columns[0]]
            + [[rotated(value, "dp", j) for value in columns[j]] for j in range(1, dp_count)]
        )
        query_list.append(query_grad)
        kept.append(partial(pair_grad, 0))
        pair_list.append(
            jnp.stack(
                [
                    lax.dynamic_slice_in_dim(pair_grad, owner_start(-k), row_count, axis=0)
                    for k in range(tensor_count)
                ]
            )
        )

    pair_local = jnp.stack(pair_list, axis=1)
    pair_all = [pair_local] + [rotated(pair_local, "dp", j) for j in range(1, dp_count)]

    def norm_back(tick, *earlier):
        normed_grad = kept[tick].astype(jnp.float32)
        for part in after(received[tick], *earlier):
            normed_grad = normed_grad + part.astype(jnp.float32)
        upcast = local_rows[tick].astype(jnp.float32)
        inverse = inverse_ticks[tick]
        scaled = normed_grad * gain_wide
        return inverse * scaled - upcast * inverse * inverse * inverse * jnp.mean(
            scaled * upcast, axis=-1, keepdims=True
        )

    outgoing = section_cotangent[0, 0].astype(jnp.float32) + norm_back(0)
    outgoing = outgoing.astype(jnp.bfloat16)
    incoming = shifted(outgoing, "section", -1)
    is_last = lax.axis_index("section") == lax.axis_size("section") - 1
    incoming = jnp.where(is_last, loss_cotangent[0], incoming)
    residual_grad = (incoming.astype(jnp.float32) + norm_back(1, outgoing)).astype(jnp.bfloat16)

    own_columns, other_ticks, pair_all = after((own_columns, other_ticks, pair_all), outgoing)

    def contract(columns, pairs):
        left = jnp.concatenate([value.reshape(-1, block_width) for value in columns])
        right = jnp.concatenate([value.reshape(-1, pair_width) for value in pairs])
        return lax.dot_general(
            left, right, (((0,), (0,)), ((), ())), preferred_element_type=jnp.float32
        )

    weight_sum = contract(own_columns, [value[0] for value in pair_all])
    if tensor_count > 1:
        others = [
            jnp.stack([jnp.stack([other_ticks[tick][j][k] for tick in ticks]) for k in range(tensor_count - 1)])
            for j in range(dp_count)
        ]
        weight_sum = weight_sum + contract(others, [value[1:] for value in pair_all])
    projection_grad = weight_sum.astype(jnp.bfloat16).reshape(1, -1, 1, 2, head_size)
    query_all = jnp.stack(query_list)[None, None]
    return (query_all, residual_grad[None, None], projection_grad)


def solution(mesh):
    in_specs = (
        P("section", "dp", None, "tensor", None),
        P("section", None),
        P("section", None, "tensor", None, None),
        P("section", "dp", None, None, "tensor", None),
        P("section", "dp", None, None, "tensor", None),
        P("section", "dp", "tensor", None),
        P("dp", "tensor", None),
        P("section", "dp", None),
        P("section", "dp", None, None),
    )
    out_specs = (
        P("section", "dp", None, None, "tensor", None),
        P("section", "dp", "tensor", None),
        P("section", "dp", "tensor", None, None),
    )


    return jax.shard_map(on_device, mesh=mesh, in_specs=in_specs, out_specs=out_specs, check_vma=False)
```

```python
import jax
import jax.numpy as jnp
from jax import lax
from jax.sharding import PartitionSpec as P


EPSILON = 1e-05
MASKED = -1e30


def shifted(value, axis, steps):
    count = lax.axis_size(axis)
    leading, last = (max(0, -steps), min(count, count - steps))
    return lax.ppermute(value, axis, [(source, source + steps) for source in range(leading, last)])


def normalize(residual, gain_wide):
    upcast = residual.astype(jnp.float32)
    inverse = lax.rsqrt(jnp.mean(upcast * upcast, axis=-1, keepdims=True) + EPSILON)
    return ((upcast * inverse * gain_wide).astype(jnp.bfloat16), inverse)


def project(rows, weights):
    return jnp.dot(rows, weights, preferred_element_type=jnp.float32).astype(jnp.bfloat16)


def head_grads(projected, query_rows, grad_rows, length, segment):
    head_size = projected.shape[1] // 2
    row_total = projected.shape[0]
    group_size = query_rows.shape[-1] // head_size
    scaling = head_size ** (-0.5)
    key_rows = projected[:, :head_size]
    value_rows = projected[:, head_size:]
    position = lax.iota(jnp.int32, row_total)
    visible = (position[None, :] <= position[:, None]) & (segment[:, None] == segment[None, :])
    live_mask = (position < length).astype(jnp.bfloat16)
    query = query_rows.reshape(row_total, group_size, head_size)
    masked_grad = grad_rows.reshape(row_total, group_size, head_size) * live_mask[:, None, None]
    scores = (
        jnp.einsum("qgd,kd->gqk", query, key_rows, preferred_element_type=jnp.float32) * scaling
    )
    scores = jnp.where(visible[None], scores, MASKED)
    row_max = jnp.max(scores, axis=-1, keepdims=True)
    exponent = jnp.exp(scores - row_max)
    attention = exponent / jnp.sum(exponent, axis=-1, keepdims=True)
    attention_low = attention.astype(jnp.bfloat16)
    mixed = jnp.einsum("gqk,kd->gqd", attention_low, value_rows, preferred_element_type=jnp.float32)
    correction = jnp.sum(mixed * jnp.transpose(masked_grad, (1, 0, 2)).astype(jnp.float32), axis=-1)
    value_grad = jnp.einsum(
        "gqk,qgd->kd", attention_low, masked_grad, preferred_element_type=jnp.float32
    )
    weight_grad = jnp.einsum(
        "qgd,kd->gqk", masked_grad, value_rows, preferred_element_type=jnp.float32
    )
    score_grad = (attention * (weight_grad - correction[..., None])).astype(jnp.bfloat16)
    query_grad = (
        jnp.einsum("gqk,kd->qgd", score_grad, key_rows, preferred_element_type=jnp.float32)
        * scaling
    ).astype(jnp.bfloat16)
    key_grad = (
        jnp.einsum("gqk,qgd->kd", score_grad, query, preferred_element_type=jnp.float32) * scaling
    )
    pair_grad = jnp.concatenate([key_grad, value_grad], axis=1).astype(jnp.bfloat16)
    return (query_grad.reshape(row_total, 1, group_size * head_size), pair_grad)


def rotated(value, axis, steps):
    count = lax.axis_size(axis)
    return lax.ppermute(value, axis, [(source, (source + steps) % count) for source in range(count)])


def after(value, *earlier):
    return lax.optimization_barrier((value, *earlier))[0]


def on_device(
    residuals,
    norm_gain,
    projection,
    queries,
    output_grad,
    section_cotangent,
    loss_cotangent,
    lengths,
    segments,
):
    local_rows = residuals[0, 0]
    tick_count, row_count, model_width = local_rows.shape
    head_size = projection.shape[4]
    pair_width = 2 * head_size
    weights = projection.reshape(model_width, pair_width)
    gain_wide = norm_gain[0].astype(jnp.float32)
    tensor_count = lax.axis_size("tensor")
    tensor_index = lax.axis_index("tensor")
    dp_count = lax.axis_size("dp")
    dp_index = lax.axis_index("dp")
    block_width = model_width // dp_count
    row_total = row_count * tensor_count
    ticks = range(tick_count)

    def owner_start(steps):
        return lax.rem(tensor_index + (tensor_count + steps), tensor_count) * row_count

    def column_block(value, steps):
        start = lax.rem(dp_index + steps, dp_count) * block_width
        return lax.dynamic_slice_in_dim(value, start, block_width, axis=value.ndim - 1)

    normed_ticks, inverse_ticks, arrived = [], [], []
    for tick in ticks:
        rows = after(local_rows[tick], *normed_ticks)
        normed, inverse = normalize(rows, gain_wide)
        normed_ticks.append(normed)
        inverse_ticks.append(inverse)
        arrived.append([rotated(normed, "tensor", k) for k in range(1, tensor_count)])
    normed_local = jnp.stack(normed_ticks)

    own_columns = [column_block(normed_local, 0)] + [
        rotated(column_block(normed_local, j), "dp", j) for j in range(1, dp_count)
    ]

    projected_own = project(normed_local.reshape(-1, model_width), weights)
    projected_own = projected_own.reshape(tick_count, row_count, pair_width)

    query_list, pair_list, received, kept = [], [], [], []
    other_ticks = []
    sent = ()
    for tick in ticks:
        gathered = after(arrived[tick], sent)
        columns = [[column_block(rows, j) for rows in gathered] for j in range(dp_count)]
        columns = lax.optimization_barrier(columns)
        if tick > 0:
            gathered = after(gathered, columns)
        pieces = [projected_own[tick]] + [project(rows, weights) for rows in gathered]
        projected = jnp.zeros((row_total, pair_width), jnp.bfloat16)
        for k, piece in enumerate(pieces):
            projected = lax.dynamic_update_slice_in_dim(projected, piece, owner_start(-k), axis=0)
        query_grad, pair_grad = head_grads(
            projected,
            queries[0, 0, tick],
            output_grad[0, 0, tick],
            lengths[0, 0, tick],
            segments[0, 0, tick],
        )

        def partial(pairs, steps):
            rows = lax.dynamic_slice_in_dim(pairs, owner_start(steps), row_count, axis=0)
            return lax.dot_general(
                rows, weights, (((1,), (1,)), ((), ())), preferred_element_type=jnp.float32
            ).astype(jnp.bfloat16)

        leaving = [partial(pair_grad, k) for k in range(1, tensor_count)]
        leaving = lax.optimization_barrier(leaving)
        received.append([rotated(value, "tensor", k + 1) for k, value in enumerate(leaving)])
        sent = (tuple(leaving), columns)
        query_grad, pair_grad = after((query_grad, pair_grad), sent)
        other_ticks.append(
            [columns[0]]
            + [[rotated(value, "dp", j) for value in columns[j]] for j in range(1, dp_count)]
        )
        query_list.append(query_grad)
        kept.append(partial(pair_grad, 0))
        pair_list.append(
            jnp.stack(
                [
                    lax.dynamic_slice_in_dim(pair_grad, owner_start(-k), row_count, axis=0)
                    for k in range(tensor_count)
                ]
            )
        )

    pair_local = [jnp.stack([pairs[k] for pairs in pair_list]) for k in range(tensor_count)]
    pair_local = lax.optimization_barrier(pair_local)
    pair_all = [pair_local] + [
        [rotated(pairs, "dp", j) for pairs in pair_local] for j in range(1, dp_count)
    ]

    def norm_back(tick, *earlier):
        normed_grad = kept[tick].astype(jnp.float32)
        for part in after(received[tick], *earlier):
            normed_grad = normed_grad + part.astype(jnp.float32)
        upcast = local_rows[tick].astype(jnp.float32)
        inverse = inverse_ticks[tick]
        scaled = normed_grad * gain_wide
        return inverse * scaled - upcast * inverse * inverse * inverse * jnp.mean(
            scaled * upcast, axis=-1, keepdims=True
        )

    outgoing = section_cotangent[0, 0].astype(jnp.float32) + norm_back(0)
    outgoing = outgoing.astype(jnp.bfloat16)
    incoming = shifted(outgoing, "section", -1)
    is_last = lax.axis_index("section") == lax.axis_size("section") - 1
    incoming = jnp.where(is_last, loss_cotangent[0], incoming)
    residual_grad = (incoming.astype(jnp.float32) + norm_back(1, outgoing)).astype(jnp.bfloat16)

    own_columns, other_ticks, pair_all = after((own_columns, other_ticks, pair_all), residual_grad)

    def contract(columns, pairs):
        left = jnp.concatenate([value.reshape(-1, block_width) for value in columns])
        right = jnp.concatenate([value.reshape(-1, pair_width) for value in pairs])
        return lax.dot_general(
            left, right, (((0,), (0,)), ((), ())), preferred_element_type=jnp.float32
        )

    weight_sum = contract(own_columns, [value[0] for value in pair_all])
    if tensor_count > 1:
        for tick in ticks:
            weight_sum = weight_sum + contract(
                [jnp.concatenate(columns) for columns in other_ticks[tick]],
                [
                    jnp.concatenate([value[tick] for value in pairs[1:]])
                    for pairs in pair_all
                ],
            )
    projection_grad = weight_sum.astype(jnp.bfloat16).reshape(1, -1, 1, 2, head_size)
    query_all = jnp.stack(query_list)[None, None]
    return (query_all, residual_grad[None, None], projection_grad)


def solution(mesh):
    in_specs = (
        P("section", "dp", None, "tensor", None),
        P("section", None),
        P("section", None, "tensor", None, None),
        P("section", "dp", None, None, "tensor", None),
        P("section", "dp", None, None, "tensor", None),
        P("section", "dp", "tensor", None),
        P("dp", "tensor", None),
        P("section", "dp", None),
        P("section", "dp", None, None),
    )
    out_specs = (
        P("section", "dp", None, None, "tensor", None),
        P("section", "dp", "tensor", None),
        P("section", "dp", "tensor", None, None),
    )


    return jax.shard_map(
        on_device, mesh=mesh, in_specs=in_specs, out_specs=out_specs, check_vma=False
    )
```
